128 devices in a mesh: data: 64 (over z, y, x), model: 2 (over core).
Axes of the slice: x: 4, y: 4, z: 4, core: 2. Of those that a mesh axis runs over, the one named last changes fastest.
Arguments:
- x_teach: bfloat16 [256, 128, 768], P('data', 'model')
- x_stud: bfloat16 [256, 128, 312], P(('data', 'model'))
- t_up: bfloat16 [24, 768, 3072], P(None, None, 'model')
- t_down: bfloat16 [24, 3072, 768], P(None, 'model')
- t_gain: float32 [24, 768], replicated
- s_up: bfloat16 [6, 312, 1248], replicated
- s_down: bfloat16 [6, 1248, 312], replicated
- s_gain_mlp: float32 [6, 312], replicated
- s_gain_proj: float32 [6, 312], replicated
- s_proj: bfloat16 [6, 312, 768], replicated
Outputs:
- output 1: float32 [], replicated
- output 2: float32 [6, 312, 1248], replicated
- output 3: float32 [6, 1248, 312], replicated
- output 4: float32 [6, 312], replicated
- output 5: float32 [6, 312], replicated
- output 6: float32 [6, 312, 768], replicated
All inputs are finite; a program needn't handle non-finite values.
Results may differ from the reference program's by a relative error of at most 0.00403566.
Values are sent between devices in bfloat16 or wider.
A program may use at most 1 GiB of HBM per device.

```python
import jax
import jax.numpy as jnp
from jax import lax

DATA_SIZE = 64
MODEL_SIZE = 2
ROWS_DEV = 2
SEQ_LEN = 128
TEACH_DIM = 768
STUD_DIM = 312
STUD_LAYERS = 6
TEACH_PER = 4

BATCH = DATA_SIZE * MODEL_SIZE * ROWS_DEV
TEACH_LAYERS = STUD_LAYERS * TEACH_PER
TEACH_FF = 4 * TEACH_DIM
STUD_FF = 4 * STUD_DIM
FF_SHARD = TEACH_FF // MODEL_SIZE
LOSS_SCALE = 1.0 / (STUD_LAYERS * BATCH * SEQ_LEN * TEACH_DIM)
NORM_EPS = 1e-6


def setup_inputs(seed: int = 0) -> dict:
    key_list = jax.random.split(jax.random.key(seed), 10)
    teach_f = jax.random.normal(key_list[0], (BATCH, SEQ_LEN, TEACH_DIM), jnp.float32)
    noise_s = jax.random.normal(key_list[1], (BATCH, SEQ_LEN, STUD_DIM), jnp.float32)
    stud_f = 0.8 * teach_f[:, :, :STUD_DIM] + 0.6 * noise_s
    t_up = jax.random.normal(key_list[2], (TEACH_LAYERS, TEACH_DIM, TEACH_FF), jnp.float32) * TEACH_DIM ** -0.5
    t_down = jax.random.normal(key_list[3], (TEACH_LAYERS, TEACH_FF, TEACH_DIM), jnp.float32) * TEACH_FF ** -0.5
    t_gain = 1.0 + 0.3 * jax.random.normal(key_list[4], (TEACH_LAYERS, TEACH_DIM), jnp.float32)
    s_up = jax.random.normal(key_list[5], (STUD_LAYERS, STUD_DIM, STUD_FF), jnp.float32) * STUD_DIM ** -0.5
    s_down = jax.random.normal(key_list[6], (STUD_LAYERS, STUD_FF, STUD_DIM), jnp.float32) * STUD_FF ** -0.5
    s_gain_mlp = 1.0 + 0.3 * jax.random.normal(key_list[7], (STUD_LAYERS, STUD_DIM), jnp.float32)
    s_gain_proj = 1.0 + 0.3 * jax.random.normal(key_list[8], (STUD_LAYERS, STUD_DIM), jnp.float32)
    s_proj = jax.random.normal(key_list[9], (STUD_LAYERS, STUD_DIM, TEACH_DIM), jnp.float32) * STUD_DIM ** -0.5
    return {
        'x_teach': teach_f.astype(jnp.bfloat16),
        'x_stud': stud_f.astype(jnp.bfloat16),
        't_up': t_up.astype(jnp.bfloat16),
        't_down': t_down.astype(jnp.bfloat16),
        't_gain': t_gain,
        's_up': s_up.astype(jnp.bfloat16),
        's_down': s_down.astype(jnp.bfloat16),
        's_gain_mlp': s_gain_mlp,
        's_gain_proj': s_gain_proj,
        's_proj': s_proj.astype(jnp.bfloat16),
    }


def rms_norm(values, gain_vec):
    widened = values.astype(jnp.float32)
    inv_rms = lax.rsqrt(jnp.mean(widened * widened, axis=-1, keepdims=True) + NORM_EPS)
    return widened * inv_rms * gain_vec


def teacher_layer(hidden, layer_w):
    up_w, down_w, gain_vec = layer_w
    normed = rms_norm(hidden, gain_vec).astype(jnp.bfloat16)
    pre_act = jnp.dot(normed, up_w, preferred_element_type=jnp.float32)
    hidden_act = jax.nn.gelu(pre_act, approximate=True).astype(jnp.bfloat16)
    act_parts = hidden_act.reshape(SEQ_LEN, MODEL_SIZE, FF_SHARD).transpose(1, 0, 2)
    down_parts = down_w.reshape(MODEL_SIZE, FF_SHARD, TEACH_DIM)

    def shard_step(acc_sum, operands):
        act_part, down_part = operands
        part_out = jnp.dot(act_part, down_part, preferred_element_type=jnp.float32)
        return acc_sum + part_out.astype(jnp.bfloat16).astype(jnp.float32), None

    summed, _ = lax.scan(shard_step, hidden.astype(jnp.float32), (act_parts, down_parts))
    return summed.astype(jnp.bfloat16), None


def teacher_feats(x_row, t_up, t_down, t_gain):
    grouped = (
        t_up.reshape(STUD_LAYERS, TEACH_PER, TEACH_DIM, TEACH_FF),
        t_down.reshape(STUD_LAYERS, TEACH_PER, TEACH_FF, TEACH_DIM),
        t_gain.reshape(STUD_LAYERS, TEACH_PER, TEACH_DIM),
    )

    def feat_step(hidden, group_w):
        hidden, _ = lax.scan(teacher_layer, hidden, group_w)
        return hidden, hidden

    _, feat_stack = lax.scan(feat_step, x_row, grouped)
    return feat_stack


def student_loss(params, x_row, feat_stack):
    def stud_block(stud_state, layer_in):
        up_w, down_w, gain_mlp, gain_proj, proj_w, feat_arr = layer_in
        normed = rms_norm(stud_state, gain_mlp).astype(jnp.bfloat16)
        pre_act = jnp.dot(normed, up_w.astype(jnp.bfloat16), preferred_element_type=jnp.float32)
        hidden_act = jax.nn.gelu(pre_act, approximate=True).astype(jnp.bfloat16)
        mlp_out = jnp.dot(hidden_act, down_w.astype(jnp.bfloat16), preferred_element_type=jnp.float32)
        new_state = (stud_state.astype(jnp.float32) + mlp_out).astype(jnp.bfloat16)
        projected = rms_norm(new_state, gain_proj).astype(jnp.bfloat16)
        diff_err = jnp.dot(projected, proj_w.astype(jnp.bfloat16), preferred_element_type=jnp.float32) - feat_arr.astype(jnp.float32)
        return new_state, jnp.sum(diff_err * diff_err)

    _, sq_sums = lax.scan(stud_block, x_row, params + (feat_stack,))
    return jnp.sum(sq_sums) * LOSS_SCALE


def reference(x_teach, x_stud, t_up, t_down, t_gain, s_up, s_down, s_gain_mlp, s_gain_proj, s_proj):
    params = (s_up.astype(jnp.float32), s_down.astype(jnp.float32), s_gain_mlp, s_gain_proj, s_proj.astype(jnp.float32))
    loss_grad = jax.value_and_grad(student_loss)

    def row_step(carry_in, rows_in):
        loss_acc, grad_acc = carry_in
        row_teach, row_stud = rows_in
        feat_stack = teacher_feats(row_teach, t_up, t_down, t_gain)
        loss_val, grad_vals = loss_grad(params, row_stud, feat_stack)
        return (loss_acc + loss_val, jax.tree.map(jnp.add, grad_acc, grad_vals)), None

    init_carry = (jnp.zeros((), jnp.float32), jax.tree.map(jnp.zeros_like, params))
    (loss_sum, grad_sum), _ = lax.scan(row_step, init_carry, (x_teach, x_stud))
    return (loss_sum, grad_sum[0], grad_sum[1], grad_sum[2], grad_sum[3], grad_sum[4])
```

```python
import functools
import jax
import jax.numpy as jnp
from jax import lax
from jax.experimental import pallas as pl
from jax.experimental.pallas import tpu as pltpu
from jax.sharding import PartitionSpec as P

NORM_EPS = 1e-6
GELU_K = 0.7978845608028654
GELU_C = 0.044715
MESH = pl.DeviceIdType.MESH
BF = jnp.bfloat16
F32 = jnp.float32


def gelu(x):
    x2 = x * x
    t = jnp.tanh(x * (GELU_K + (GELU_K * GELU_C) * x2))
    hx = 0.5 * x
    return hx + hx * t


def gelu_grad(x):
    x2 = x * x
    t = jnp.tanh(x * (GELU_K + (GELU_K * GELU_C) * x2))
    inner = GELU_K + (3.0 * GELU_K * GELU_C) * x2
    return 0.5 * (1.0 + t) + (0.5 * x) * (1.0 - t * t) * inner


def inv_rms(w):
    return lax.rsqrt(jnp.mean(w * w, axis=-1, keepdims=True) + NORM_EPS)


def dot(a, b):
    return jnp.dot(a, b, preferred_element_type=F32)


def dot_tn(a, b):
    return lax.dot_general(a, b, (((0,), (0,)), ((), ())), preferred_element_type=F32)


def dot_nt(a, b):
    return lax.dot_general(a, b, (((1,), (1,)), ((), ())), preferred_element_type=F32)


def teacher_kernel(per_feat, x_ref, gain_ref, up_hbm, down_hbm, feat_ref, h, a, u, own, peer, upb, downb, wsem, xsem, ssem, rsem):
    core = lax.axis_index('model')
    other = 1 - core
    n_layers = up_hbm.shape[0]
    n_chunk, rows, dim = h.shape
    ff = upb.shape[2]
    half = x_ref.shape[1]
    sub = 32

    def up_copy(layer, slot):
        return pltpu.make_async_copy(up_hbm.at[layer], upb.at[slot], wsem.at[slot, 0])

    def down_copy(layer, slot):
        return pltpu.make_async_copy(down_hbm.at[layer], downb.at[slot], wsem.at[slot, 1])

    def exchange(chunk, slot):
        return pltpu.make_async_remote_copy(
            src_ref=own.at[chunk], dst_ref=peer.at[slot, chunk], send_sem=ssem.at[chunk], recv_sem=rsem.at[slot, chunk],
            device_id={'model': other}, device_id_type=MESH)

    up_copy(0, 0).start()
    down_copy(0, 0).start()
    barrier = pltpu.get_barrier_semaphore()
    pl.semaphore_signal(barrier, inc=1, device_id={'model': other}, device_id_type=MESH)
    pl.semaphore_wait(barrier, 1)
    mine = pl.ds(pl.multiple_of(core * half, half), half)
    x_copy = pltpu.make_async_remote_copy(
        src_ref=x_ref, dst_ref=h.at[:, mine, :], send_sem=xsem.at[0], recv_sem=xsem.at[1],
        device_id={'model': other}, device_id_type=MESH)
    x_copy.start()
    h[:, mine, :] = x_ref[...]
    own[...] = jnp.zeros_like(own)
    peer[1] = jnp.zeros(peer.shape[1:], BF)

    def combine(chunk, slot, gain_row):
        for r in range(0, rows, sub):
            sl = pl.ds(r, sub)
            w = h[chunk, sl, :].astype(F32) + (own[chunk, sl, :].astype(F32) + peer[slot, chunk, sl, :].astype(F32))
            hb = w.astype(BF)
            h[chunk, sl, :] = hb
            w = hb.astype(F32)
            a[chunk, sl, :] = (w * inv_rms(w) * gain_row).astype(BF)

    x_copy.wait()
    combine(0, 1, gain_ref[pl.ds(0, 1), :])

    def keep(layer, chunk):
        @pl.when((lax.rem(layer + 1, per_feat) == 0) & (core == chunk // 2))
        def _():
            feat_ref[layer // per_feat, chunk % 2] = h[chunk]

    def layer_step(layer, carry):
        slot = lax.rem(layer, 2)
        prev = 1 - slot

        @pl.when(layer + 1 < n_layers)
        def _():
            up_copy(layer + 1, prev).start()
            down_copy(layer + 1, prev).start()

        up_copy(layer, slot).wait()
        down_copy(layer, slot).wait()
        for chunk in range(n_chunk):
            nxt = (chunk + 1) % n_chunk
            if nxt:
                @pl.when(layer > 0)
                def _():
                    exchange(nxt, prev).wait()
                src, gain_at = prev, layer
            else:
                exchange(nxt, slot).wait()
                src, gain_at = slot, jnp.minimum(layer + 1, n_layers - 1)
            gain_row = gain_ref[pl.ds(gain_at, 1), :]
            act = a[chunk]
            for n in range(0, ff, 512):
                u[chunk % 2, :, n:n + 512] = gelu(dot(act, upb[slot, :, n:n + 512])).astype(BF)
            own[chunk] = dot(u[chunk % 2], downb[slot]).astype(BF)
            combine(nxt, src, gain_row)
            exchange(chunk, slot).start()
            if nxt:
                @pl.when(layer > 0)
                def _():
                    keep(layer - 1, nxt)
            else:
                keep(layer, nxt)
        return carry

    lax.fori_loop(0, n_layers, layer_step, 0)
    last = (n_layers - 1) % 2
    for chunk in range(1, n_chunk):
        exchange(chunk, last).wait()
        combine(chunk, last, gain_ref[pl.ds(0, 1), :])
        keep(n_layers - 1, chunk)


def teacher(x_loc, up_loc, down_loc, gain, n_feat):
    n_chunk, half, dim = x_loc.shape
    n_layers, _, ff = up_loc.shape
    rows = 2 * half
    flops = 4 * n_layers * n_chunk * rows * dim * ff
    vmem = pl.BlockSpec(memory_space=pltpu.VMEM)
    hbm = pl.BlockSpec(memory_space=pl.ANY)
    return pl.pallas_call(
        functools.partial(teacher_kernel, n_layers // n_feat),
        out_shape=jax.ShapeDtypeStruct((n_feat, n_chunk // 2, rows, dim), BF),
        in_specs=[vmem, vmem, hbm, hbm],
        out_specs=vmem,
        scratch_shapes=[
            pltpu.VMEM((n_chunk, rows, dim), BF),
            pltpu.VMEM((n_chunk, rows, dim), BF),
            pltpu.VMEM((2, rows, ff), BF),
            pltpu.VMEM((n_chunk, rows, dim), BF),
            pltpu.VMEM((2, n_chunk, rows, dim), BF),
            pltpu.VMEM((2, dim, ff), BF),
            pltpu.VMEM((2, ff, dim), BF),
            pltpu.SemaphoreType.DMA((2, 2)),
            pltpu.SemaphoreType.DMA((2,)),
            pltpu.SemaphoreType.DMA((n_chunk,)),
            pltpu.SemaphoreType.DMA((2, n_chunk)),
        ],
        compiler_params=pltpu.CompilerParams(collective_id=0, has_side_effects=True, vmem_limit_bytes=60 * 1024 * 1024),
        cost_estimate=pl.CostEstimate(flops=flops, bytes_accessed=2 * n_layers * dim * ff * 2, transcendentals=n_layers * n_chunk * rows * ff),
        name='teacher',
    )(x_loc, gain, up_loc, down_loc)


def student_kernel(loss_scale, x_ref, gm_ref, gp_ref, feat_hbm, up_hbm, down_hbm, proj_hbm, gup_hbm, gdown_hbm, gproj_hbm, small_ref,
                   st, nm, ha, pj, de, pre, gs, upb, downb, projb, featb, gub, gdb, gpb, wsem, osem):
    n_layers, dim, ff = up_hbm.shape
    tdim = proj_hbm.shape[2]
    cuts = [(n, min(n + 512, ff)) for n in range(0, ff, 512)]

    def loads(j):
        return [pltpu.make_async_copy(src.at[j], dst.at[j], wsem.at[j, i])
                for i, (src, dst) in enumerate(((up_hbm, upb), (down_hbm, downb), (proj_hbm, projb), (feat_hbm, featb)))]

    def stores(j, slot):
        return [pltpu.make_async_copy(src.at[slot], dst.at[j], osem.at[slot, i])
                for i, (src, dst) in enumerate(((gpb, gproj_hbm), (gdb, gdown_hbm), (gub, gup_hbm)))]

    for j in range(n_layers):
        for cp in loads(j):
            cp.start()
    for r in range(x_ref.shape[0]):
        st[0, r * x_ref.shape[2]:(r + 1) * x_ref.shape[2], :] = x_ref[r].astype(F32).T.astype(BF)
    small_ref[...] = jnp.zeros_like(small_ref)

    def fwd(j, carry):
        for cp in loads(j):
            cp.wait()
        w = st[j].astype(F32)
        normed = (w * inv_rms(w) * gm_ref[pl.ds(j, 1), :]).astype(BF)
        nm[j] = normed
        for lo, hi in cuts:
            p = dot(normed, upb[j, :, lo:hi])
            pre[j, :, lo:hi] = p
            ha[j, :, lo:hi] = gelu(p).astype(BF)
        s1 = (w + dot_nt(ha[j], downb[j])).astype(BF)
        st[j + 1] = s1
        w1 = s1.astype(F32)
        projected = (w1 * inv_rms(w1) * gp_ref[pl.ds(j, 1), :]).astype(BF)
        pj[j] = projected
        for lo in range(0, tdim, 256):
            hi = lo + 256
            e = dot(projected, projb[j, :, lo:hi]) - featb[j, :, lo:hi].astype(F32)
            small_ref[pl.ds(12, 1), lo:hi] += jnp.sum(e * e, axis=0, keepdims=True) * loss_scale
            de[j, :, lo:hi] = ((2.0 * loss_scale) * e).astype(BF)
        return carry

    lax.fori_loop(0, n_layers, fwd, 0)
    gs[...] = jnp.zeros_like(gs)

    def bwd(i, carry):
        j = n_layers - 1 - i
        slot = lax.rem(i, 2)

        @pl.when(i >= 2)
        def _():
            for cp in stores(j, slot):
                cp.wait()
        st_proj, st_down, st_up = stores(j, slot)
        d_err = de[j]
        d_projected = dot_nt(d_err, projb[j])
        gpb[slot] = dot_tn(pj[j], d_err)
        w1 = st[j + 1].astype(F32)
        inv1 = inv_rms(w1)
        unit1 = w1 * inv1
        small_ref[pl.ds(6 + j, 1), 0:dim] = jnp.sum(d_projected * unit1, axis=0, keepdims=True)
        gu = d_projected * gp_ref[pl.ds(j, 1), :]
        g = gs[...] + inv1 * (gu - unit1 * jnp.mean(gu * unit1, axis=-1, keepdims=True))
        d_state = g.astype(BF)
        st_proj.start()
        for lo, hi in cuts:
            d_act = dot(d_state, downb[j, :, lo:hi])
            ha_cut = ha[j, :, lo:hi]
            d_pre = (gelu_grad(pre[j, :, lo:hi]) * d_act).astype(BF)
            gdb[slot, :, lo:hi] = dot_tn(d_state, ha_cut)
            ha[j, :, lo:hi] = d_pre
        st_down.start()
        d_normed = dot_nt(ha[j], upb[j])
        for lo, hi in cuts:
            gub[slot, :, lo:hi] = dot_tn(nm[j], ha[j, :, lo:hi])
        st_up.start()
        w = st[j].astype(F32)
        inv0 = inv_rms(w)
        unit0 = w * inv0
        small_ref[pl.ds(j, 1), 0:dim] = jnp.sum(d_normed * unit0, axis=0, keepdims=True)
        gu = d_normed * gm_ref[pl.ds(j, 1), :]
        gs[...] = g + inv0 * (gu - unit0 * jnp.mean(gu * unit0, axis=-1, keepdims=True))
        return carry

    lax.fori_loop(0, n_layers, bwd, 0)
    for slot in range(2):
        for cp in stores(0, slot):
            cp.wait()


def student(x, feats, up_s, down_s, gm, gp, proj_s, loss_scale):
    n_layers, dim, ff = up_s.shape
    tokens = x.shape[0] * x.shape[2]
    tdim = proj_s.shape[2]
    vmem = pl.BlockSpec(memory_space=pltpu.VMEM)
    hbm = pl.BlockSpec(memory_space=pl.ANY)
    flops = 6 * tokens * n_layers * dim * (2 * ff + tdim)
    return pl.pallas_call(
        functools.partial(student_kernel, loss_scale),
        out_shape=(
            jax.ShapeDtypeStruct(up_s.shape, F32),
            jax.ShapeDtypeStruct(down_s.shape, F32),
            jax.ShapeDtypeStruct(proj_s.shape, F32),
            jax.ShapeDtypeStruct((16, tdim), F32),
        ),
        in_specs=[vmem, vmem, vmem, hbm, hbm, hbm, hbm],
        out_specs=(hbm, hbm, hbm, vmem),
        scratch_shapes=[
            pltpu.VMEM((n_layers + 1, tokens, dim), BF),
            pltpu.VMEM((n_layers, tokens, dim), BF),
            pltpu.VMEM((n_layers, tokens, ff), BF),
            pltpu.VMEM((n_layers, tokens, dim), BF),
            pltpu.VMEM((n_layers, tokens, tdim), BF),
            pltpu.VMEM((n_layers, tokens, ff), F32),
            pltpu.VMEM((tokens, dim), F32),
            pltpu.VMEM(up_s.shape, BF),
            pltpu.VMEM(down_s.shape, BF),
            pltpu.VMEM(proj_s.shape, BF),
            pltpu.VMEM((n_layers, tokens, tdim), BF),
            pltpu.VMEM((2,) + up_s.shape[1:], F32),
            pltpu.VMEM((2,) + down_s.shape[1:], F32),
            pltpu.VMEM((2,) + proj_s.shape[1:], F32),
            pltpu.SemaphoreType.DMA((n_layers, 4)),
            pltpu.SemaphoreType.DMA((2, 3)),
        ],
        compiler_params=pltpu.CompilerParams(vmem_limit_bytes=60 * 1024 * 1024),
        cost_estimate=pl.CostEstimate(flops=flops, bytes_accessed=40 * 1024 * 1024, transcendentals=2 * n_layers * tokens * ff),
        name='student',
    )(x, gm, gp, feats, up_s, down_s, proj_s)


def solution(mesh):
    spec_list = (P('data', 'model', None), P(('data', 'model'), None, None), P(None, None, 'model'), P(None, 'model', None), P(), P(), P(), P(), P(), P())

    def distill_step(x_teach, x_stud, t_up, t_down, t_gain, s_up, s_down, s_gain_mlp, s_gain_proj, s_proj):
        n_feat = s_up.shape[0]
        loss_scale = 1.0 / (n_feat * x_teach.shape[0] * x_teach.shape[1] * x_teach.shape[2])

        def local_fn(teach_loc, stud_loc, up_loc, down_loc, gain_t, up_s, down_s, gain_mlp, gain_proj, proj_s):
            dim = stud_loc.shape[2]
            tokens = stud_loc.shape[0] * stud_loc.shape[1]
            feats = teacher(teach_loc, up_loc, down_loc, gain_t, n_feat).reshape(n_feat, tokens, -1)
            g_up, g_down, g_proj, small = student(jnp.swapaxes(stud_loc, 1, 2), feats, up_s, jnp.swapaxes(down_s, 1, 2), gain_mlp, gain_proj, proj_s, loss_scale)
            g_up, g_down, g_proj, small = lax.psum((g_up, g_down, g_proj, small), ('data', 'model'))
            return jnp.sum(small[12]), g_up, jnp.swapaxes(g_down, 1, 2), small[0:6, :dim], small[6:12, :dim], g_proj

        mapped = jax.shard_map(local_fn, mesh=mesh, in_specs=spec_list, out_specs=(P(),) * 6, check_vma=False)
        return mapped(x_teach, x_stud, t_up, t_down, t_gain, s_up, s_down, s_gain_mlp, s_gain_proj, s_proj)

    return distill_step
```
